256 devices in a mesh: section: 2 (over x_lo), tp: 8 (over y, core), ctx: 16 (over x_hi, z).
Axes of the slice: x: 4 (x_hi: 2, x_lo: 2; x = x_hi * 2 + x_lo), y: 4, z: 8, core: 2. Of those that a mesh axis runs over, the one named last changes fastest.
Arguments:
- tokens_in: bfloat16 [2, 32, 16384], P(None, None, 'ctx'), may hold values from -6 to 6
- norm_gain: bfloat16 [2, 16384], P('section', 'ctx'), may hold values from 0.25 to 1.75
- w_qkv: bfloat16 [2, 16384, 18432], P('section', 'ctx', 'tp'), may hold values from -0.375 to 0.375
- w_out: bfloat16 [2, 16384, 16384], P('section', 'tp', 'ctx'), may hold values from -0.046875 to 0.046875
- prefix_keys: bfloat16 [2, 8, 65536, 128], P('section', 'tp', 'ctx'), may hold values from -400 to 400
- prefix_values: bfloat16 [2, 8, 65536, 128], P('section', 'tp', 'ctx'), may hold values from -6 to 6
- suffix_keys: bfloat16 [2, 8, 32, 512, 128], P('section', 'tp', 'ctx'), may hold values from -27 to 27
- suffix_values: bfloat16 [2, 8, 32, 512, 128], P('section', 'tp', 'ctx'), may hold values from -6 to 6
- lengths: int32 [32], replicated, may hold values from 1 to 512, 8192 in all
- order: int32 [32], replicated, may hold values from 0 to 31, each once
Outputs:
- layer_out: float32 [2, 2, 32, 16384], P('section', None, 'tp', 'ctx')
The draws below stay inside these ranges and needn't reach their ends.
Inputs may be any that keep to these rules, and one draw needn't show every extreme that they name: `lengths`: some sample has 512. `order`: each sample appears in exactly one row.
All inputs are finite; a program needn't handle non-finite values.
Results may differ from the reference program's by a relative error of at most 0.014.
Values may be sent and summed in bfloat16 or wider, within the bound.
A program may use at most 128 MiB of HBM per device.

```python
import math
import jax
import jax.numpy as jnp
import numpy as np
from jax import lax

D = 16384
HEADS = 128
KVH = 8
HD = 128
SMAX = 512
G = 16
LAYERS = 2
B = 32
PREFIX = 65536


def draw_w_qkv(key, part):
    group = (HEADS // KVH + 2) * HD
    column = jnp.arange(KVH * group) % group
    query_cols = HEADS // KVH * HD
    column_scale = jnp.where((column >= query_cols) & (column < query_cols + HD), 8.0, 1.0)
    shape = (LAYERS, D, KVH * group)
    base = jnp.clip(jax.random.normal(key, shape, jnp.float32), -6.0, 6.0)
    return (base * column_scale[None, None, :] * D ** (-0.5)).astype(jnp.bfloat16)


def draw_prefix_keys(key, part):
    shape = (LAYERS, KVH, PREFIX, HD)
    key_base = jax.random.fold_in(key, 11)
    base = jnp.clip(jax.random.normal(key_base, shape, jnp.float32), -6.0, 6.0) * 2.5
    return base.astype(jnp.bfloat16)


def shard_levels(own_key, dims, pieces, smallest, largest):
    level = 1.0
    for dim, shards_of in pieces:
        steps = jax.random.uniform(jax.random.fold_in(jax.random.fold_in(own_key, 6), dim), (shards_of,), jnp.float32, smallest / len(pieces), largest / len(pieces))
        level = level * jnp.repeat(jnp.exp(steps), dims[dim] // shards_of).reshape((-1,) + (1,) * (len(dims) - 1 - dim))
    return level


def split_up(amount, total, reach, slope):
    loads = [(1 << 20) // math.isqrt(grade ** slope) + 1 for grade in range(2, amount + 1)]
    spare, holding = total - reach - (amount - 1), [1] * (amount - 1)
    while spare > 0:
        free = [i for i in range(amount - 1) if holding[i] < reach]
        pool, left = sum([loads[i] for i in free]), spare
        for i in free:
            extra = min(reach - holding[i], max(1, left * loads[i] // pool), spare)
            holding[i] = holding[i] + extra
            spare = spare - extra
    return np.array([reach] + holding)


def uneven(rng, amount, total, limit, skew):
    if amount == 2:
        one = jax.random.randint(rng, (), max(1, total - limit), min(limit, total - 1) + 1)
        return jnp.stack([one, total - one])
    sizes = jnp.asarray(split_up(amount, total, limit, skew), jnp.int32)
    twos = (amount - 1) // 2
    source_of, sink = sizes[1:1 + 2 * twos:2], sizes[2:2 + 2 * twos:2]
    room = jnp.minimum(source_of - 1, limit - sink)
    moved = jax.random.randint(jax.random.fold_in(rng, 1), (twos,), 0, 1 << 20) % (room + 1)
    sizes = sizes.at[1:1 + 2 * twos:2].set(source_of - moved).at[2:2 + 2 * twos:2].set(sink + moved)
    return sizes[jax.random.permutation(jax.random.fold_in(rng, 2), amount)]


def normal_values(own_key, dims, scale, limit, split=(), held_as=jnp.bfloat16):
    factor_of = shard_levels(own_key, dims, split, -0.22, 0.18) if split else 1.0
    drawn = jax.random.normal(own_key, dims, jnp.float32) * scale * factor_of
    return jnp.minimum(jnp.maximum(drawn, -limit), limit).astype(held_as)


def setup_inputs(seed: int = 0) -> dict:
    arg_keys = jax.random.split(jax.random.key(seed), 11)
    return {
        "tokens_in": normal_values(arg_keys[0], (2, B, D), 1.0, 6.0, ((2, 16),)),
        "norm_gain": jnp.clip(1.0 + 0.15 * jax.random.normal(arg_keys[1], (LAYERS, D), jnp.float32), 0.25, 1.75).astype(jnp.bfloat16),
        "w_qkv": draw_w_qkv(jax.random.fold_in(arg_keys[10], 71), 0),
        "w_out": normal_values(arg_keys[3], (LAYERS, HEADS * HD, D), (HEADS * HD) ** -0.5, 0.046875, ((0, 2), (1, 8), (2, 16))),
        "prefix_keys": draw_prefix_keys(jax.random.fold_in(arg_keys[10], 71), 0),
        "prefix_values": normal_values(arg_keys[5], (LAYERS, KVH, PREFIX, HD), 1.0, 6.0, ((0, 2), (1, 8), (2, 16))),
        "suffix_keys": normal_values(arg_keys[6], (LAYERS, KVH, B, SMAX, HD), 4.5, 27.0, ((0, 2), (1, 8), (2, 16))),
        "suffix_values": normal_values(arg_keys[7], (LAYERS, KVH, B, SMAX, HD), 1.0, 6.0, ((0, 2), (1, 8), (2, 16))),
        "lengths": uneven(arg_keys[8], B, B * SMAX // 2, SMAX, 2).astype(jnp.int32),
        "order": jax.random.permutation(arg_keys[9], B).astype(jnp.int32),
    }


EPSILON = 1e-05
NEGATIVE = -1e+30

def rounded(values):
    return lax.optimization_barrier(values.astype(jnp.bfloat16)).astype(jnp.float32)

def apply_layer(hidden, layer_index, norm_gain, w_qkv, w_out, prefix_keys, prefix_values, suffix_keys, suffix_values, in_suffix, order, previous):
    row_count = hidden.shape[0]
    hidden_f = hidden.astype(jnp.float32)
    mean_sq = lax.optimization_barrier(jnp.mean(hidden_f * hidden_f, axis=1))
    scaled = (hidden_f * norm_gain[layer_index].astype(jnp.float32)[None, :]).astype(jnp.bfloat16)
    projected = jnp.dot(scaled, w_qkv[layer_index], preferred_element_type=jnp.float32) * lax.rsqrt(mean_sq + EPSILON)[:, None]
    projected = projected.astype(jnp.bfloat16).reshape(row_count, KVH, G + 2, HD)
    queries = projected[:, :, :G].transpose(1, 0, 2, 3)
    keys_new = projected[:, :, G].transpose(1, 0, 2)
    values_new = projected[:, :, G + 1].transpose(1, 0, 2)
    suffix_k = suffix_keys[layer_index][:, order]
    suffix_v = suffix_values[layer_index][:, order]
    has_old = previous is not None
    keys_old = previous[0] if has_old else keys_new
    values_old = previous[1] if has_old else values_new
    score_scale = HD ** (-0.5)

    def per_head(head_inputs):
        query_h, pre_k, pre_v, suf_k, suf_v, new_k, new_v, old_k, old_v = head_inputs
        query_f = query_h.astype(jnp.float32)
        pre_scores = jnp.einsum('bgd,pd->bgp', query_f, pre_k.astype(jnp.float32)) * score_scale
        suf_scores = jnp.einsum('bgd,bpd->bgp', query_f, suf_k.astype(jnp.float32)) * score_scale
        suf_scores = jnp.where(in_suffix[:, None, :], suf_scores, NEGATIVE)
        own_scores = jnp.einsum('bgd,bd->bg', query_f, new_k.astype(jnp.float32)) * score_scale
        row_max = jnp.maximum(jnp.maximum(lax.optimization_barrier(jnp.max(pre_scores, axis=2)), lax.optimization_barrier(jnp.max(suf_scores, axis=2))), own_scores)
        if has_old:
            old_scores = jnp.einsum('bgd,bd->bg', query_f, old_k.astype(jnp.float32)) * score_scale
            row_max = jnp.maximum(row_max, old_scores)
        pre_w = jnp.exp(pre_scores - row_max[..., None])
        suf_w = jnp.where(in_suffix[:, None, :], jnp.exp(suf_scores - row_max[..., None]), 0.0)
        own_w = jnp.exp(own_scores - row_max)
        totals = lax.optimization_barrier(jnp.sum(pre_w, axis=2)) + lax.optimization_barrier(jnp.sum(suf_w, axis=2)) + own_w
        summed = jnp.einsum('bgp,pd->bgd', rounded(pre_w), pre_v.astype(jnp.float32))
        summed = summed + jnp.einsum('bgp,bpd->bgd', rounded(suf_w), suf_v.astype(jnp.float32))
        summed = summed + rounded(own_w)[..., None] * new_v.astype(jnp.float32)[:, None, :]
        if has_old:
            old_w = jnp.exp(old_scores - row_max)
            totals = totals + old_w
            summed = summed + rounded(old_w)[..., None] * old_v.astype(jnp.float32)[:, None, :]
        return summed / totals[..., None]
    attention = lax.map(per_head, (queries, prefix_keys[layer_index], prefix_values[layer_index], suffix_k, suffix_v, keys_new, values_new, keys_old, values_old))
    attention = attention.transpose(1, 0, 2, 3).reshape(row_count, HEADS * HD).astype(jnp.bfloat16)
    output = jnp.dot(attention, w_out[layer_index], preferred_element_type=jnp.float32)
    return (hidden_f + output, (keys_new, values_new))

def reference(tokens_in, norm_gain, w_qkv, w_out, prefix_keys, prefix_values, suffix_keys, suffix_values, lengths, order):
    sample_len = lengths[order]
    in_suffix = jnp.arange(SMAX, dtype=jnp.int32)[None, :] < sample_len[:, None]
    results = [[] for layer_index in range(LAYERS)]
    previous = [None] * LAYERS
    for step_index in range(2):
        hidden = tokens_in[step_index].astype(jnp.float32)
        for layer_index in range(LAYERS):
            hidden, fresh = apply_layer(hidden, layer_index, norm_gain, w_qkv, w_out, prefix_keys, prefix_values, suffix_keys, suffix_values, in_suffix, order, previous[layer_index])
            previous[layer_index] = fresh
            results[layer_index].append(hidden)
    return jnp.stack([jnp.stack(entries) for entries in results])
```

```python
import functools
import math

import jax
import jax.numpy as jnp
from jax import lax
from jax.experimental import pallas as pl
from jax.experimental.pallas import tpu as pltpu
from jax.sharding import PartitionSpec as P

HD = 128
LANES = 128
STEPS = 2
EPSILON = 1e-05
NEGATIVE = -1e30
SCALE2 = HD ** (-0.5) * math.log2(math.e)
HEADS_PER_BLOCK = 4
F32 = jnp.float32
BF16 = jnp.bfloat16


def iota(shape, dim):
    return lax.broadcasted_iota(jnp.int32, shape, dim)


def column_to_row(column):
    rows = column.shape[0]
    picked = jnp.where(iota((rows, LANES), 0) == iota((rows, LANES), 1), column, 0.0)
    return jnp.sum(picked, axis=0, keepdims=True)


def row_to_column(row, rows):
    spread = jnp.broadcast_to(row, (rows, LANES))
    picked = jnp.where(iota((rows, LANES), 0) == iota((rows, LANES), 1), spread, 0.0)
    return jnp.sum(picked, axis=1, keepdims=True)


def in_three(row):
    high = row.astype(BF16).astype(F32)
    rest = row - high
    middle = rest.astype(BF16).astype(F32)
    low = rest - middle
    which = iota((8, LANES), 0)
    block = jnp.where(which == 0, jnp.broadcast_to(high, (8, LANES)), 0.0)
    block = jnp.where(which == 1, jnp.broadcast_to(middle, (8, LANES)), block)
    return jnp.where(which == 2, jnp.broadcast_to(low, (8, LANES)), block)


def kernel(
    nc,
    nt,
    tokens,
    gain,
    w_qkv,
    w_out,
    pre_keys,
    pre_values,
    suf_keys,
    suf_values,
    lengths,
    order,
    out,
    tok_v,
    gain_v,
    gain_next,
    wq_v,
    wo_v,
    k_v,
    vx,
    xg,
    x_res,
    ssb,
    p1,
    r1,
    scales,
    p2,
    r2,
    order_v,
    new_bias,
    s_v,
    p3,
    r3,
    p4,
    a4,
    p5,
    r5,
    xg6,
    ss6,
    xn6,
    load_sem,
    wq_sem,
    send_c,
    recv_c,
    send_t,
    recv_t,
    send_x,
    recv_x,
    send_g,
    recv_g,
):
    sec = lax.axis_index("section")
    tp = lax.axis_index("tp")
    ctx = lax.axis_index("ctx")
    rows = 8 * nt
    heads = nc
    model = wq_v.shape[0]
    prefix = pre_keys.shape[2]
    slots, smax = suf_keys.shape[2], suf_keys.shape[3]
    width = wo_v.shape[1]
    features = model * nc
    new_at = prefix + slots * smax
    tiles = wq_sem.shape[0]

    def load(source, target, k):
        return pltpu.make_async_copy(source, target, load_sem.at[k])

    def load_wq(n):
        cols = pl.ds(n * 256, 256)
        return pltpu.make_async_copy(
            w_qkv.at[0, :, cols], wq_v.at[:, cols], wq_sem.at[n]
        )

    barrier = pltpu.get_barrier_semaphore()

    def greet_ctx(k, carry):
        pl.semaphore_signal(barrier, inc=1, device_id={"ctx": lax.rem(ctx + k, nc)})
        return carry

    def greet_tp(k, carry):
        pl.semaphore_signal(barrier, inc=1, device_id={"tp": lax.rem(tp + k, nt)})
        return carry

    def greet_section(k, carry):
        pl.semaphore_signal(barrier, inc=1, device_id={"section": 1 - sec, "tp": k})
        return carry

    lax.fori_loop(1, nc, greet_ctx, 0)
    lax.fori_loop(1, nt, greet_tp, 0)
    lax.fori_loop(0, nt, greet_section, 0)

    loads = [
        load(tokens, tok_v, 0),
        load(gain, gain_v, 1),
    ]
    for copy in loads:
        copy.start()
    for n in [tiles - 1] + list(range(tiles - 1)):
        load_wq(n).start()
    later = [
        load(pre_keys.at[0, 0], k_v.at[pl.ds(0, prefix)], 2),
        load(pre_values.at[0, 0], vx.at[pl.ds(0, prefix), pl.ds(0, HD)], 3),
    ]
    for i in range(slots):
        at = pl.ds(prefix + i * smax, smax)
        later.append(load(suf_keys.at[0, 0, i], k_v.at[at], 4 + 2 * i))
        later.append(load(suf_values.at[0, 0, i], vx.at[at, pl.ds(0, HD)], 5 + 2 * i))
    out_load = load(w_out.at[0], wo_v, 4 + 2 * slots)
    for copy in later:
        copy.start()
    out_load.start()

    vx[:, HD:] = jnp.ones((vx.shape[0], HD), BF16)
    spare = k_v.shape[0] - new_at - rows
    k_v[pl.ds(new_at + rows, spare), :] = jnp.zeros((spare, HD), BF16)
    vx[pl.ds(new_at + rows, spare), pl.ds(0, HD)] = jnp.zeros((spare, HD), BF16)
    row_of = iota((rows, LANES), 0)
    lane_of = iota((rows, LANES), 1)
    batch_row = ((row_of >> 3) << 2) + (row_of & 3)
    sample = jnp.zeros((rows, LANES), jnp.int32)
    for r in range(rows // STEPS):
        sample = jnp.where(batch_row == r, order[r], sample)
    second = (row_of & 4) == 4
    mine = (row_of & (nc - 1)) == ctx
    allowed = mine & ((lane_of == row_of) | (second & (lane_of == row_of - 4)))
    bias = jnp.where(allowed, 0.0, NEGATIVE)
    for hh in range(HEADS_PER_BLOCK):
        order_v[pl.ds(hh * rows, rows), :] = sample
        new_bias[pl.ds(hh * rows, rows), :] = bias

    for copy in loads:
        copy.wait()

    @pl.when(sec == 0)
    def _():
        g = gain_v[...].astype(F32)
        for j in range(nt):
            x8 = jnp.concatenate(
                [tok_v[t, pl.ds(4 * j, 4), :].astype(F32) for t in range(STEPS)], axis=0
            )
            xg[j] = (x8 * g).astype(BF16)
            total = jnp.sum(x8 * x8, axis=1, keepdims=True)
            ssb[j] = jnp.broadcast_to(total, (8, LANES))

            @pl.when(tp == j)
            def _():
                x_res[...] = x8

    pl.semaphore_wait(barrier, nc - 1 + nt - 1 + nt)

    gain_copy = pltpu.make_async_remote_copy(
        src_ref=gain_v,
        dst_ref=gain_next,
        send_sem=send_g,
        recv_sem=recv_g,
        device_id={"section": 1 - sec},
    )

    def row_copies(k):
        return [
            pltpu.make_async_remote_copy(
                src_ref=xg6,
                dst_ref=xg.at[tp],
                send_sem=send_x.at[0, k],
                recv_sem=recv_x.at[0, tp],
                device_id={"section": 1 - sec, "tp": k},
            ),
            pltpu.make_async_remote_copy(
                src_ref=ss6,
                dst_ref=ssb.at[tp],
                send_sem=send_x.at[1, k],
                recv_sem=recv_x.at[1, tp],
                device_id={"section": 1 - sec, "tp": k},
            ),
        ]

    def row_arrivals(j):
        return [
            pltpu.make_async_remote_copy(
                src_ref=xg.at[j],
                dst_ref=xg.at[j],
                send_sem=send_x.at[0, j],
                recv_sem=recv_x.at[0, j],
                device_id={"section": 1 - sec, "tp": j},
            ),
            pltpu.make_async_remote_copy(
                src_ref=ssb.at[j],
                dst_ref=ssb.at[j],
                send_sem=send_x.at[1, j],
                recv_sem=recv_x.at[1, j],
                device_id={"section": 1 - sec, "tp": j},
            ),
        ]

    rest_copy = pltpu.make_async_remote_copy(
        src_ref=xn6,
        dst_ref=x_res,
        send_sem=send_x.at[2, 0],
        recv_sem=recv_x.at[2, 0],
        device_id={"section": 1 - sec},
    )

    @pl.when(sec == 1)
    def _():
        gain_copy.start()

        def arrive(j, carry):
            for copy in row_arrivals(j):
                copy.wait_recv()
            return carry

        lax.fori_loop(0, nt, arrive, 0)
        gain_copy.wait_send()

    def exchange(phase, source, target):
        def send(d):
            return pltpu.make_async_remote_copy(
                src_ref=source(d),
                dst_ref=target(ctx),
                send_sem=send_c.at[phase, d],
                recv_sem=recv_c.at[phase, ctx],
                device_id={"ctx": d},
            )

        def arrival(d):
            return pltpu.make_async_remote_copy(
                src_ref=target(d),
                dst_ref=target(d),
                send_sem=send_c.at[phase, d],
                recv_sem=recv_c.at[phase, d],
                device_id={"ctx": d},
            )

        def start_all():
            def start(k, carry):
                send(lax.rem(ctx + k, nc)).start()
                return carry

            lax.fori_loop(1, nc, start, 0)

        def wait_all():
            def wait(k, carry):
                arrival(lax.rem(ctx + k, nc)).wait_recv()
                return carry

            lax.fori_loop(1, nc, wait, 0)

        def drain():
            def wait(k, carry):
                send(lax.rem(ctx + k, nc)).wait_send()
                return carry

            lax.fori_loop(1, nc, wait, 0)

        return send, start_all, wait_all, drain

    _, start1, wait1, drain1 = exchange(0, lambda d: p1.at[d], lambda d: r1.at[d])
    xgv = xg[...].reshape(rows, model)
    squares = in_three(column_to_row(ssb[...].reshape(rows, LANES)))
    load_wq(tiles - 1).wait()
    kv = jnp.dot(xgv, wq_v[:, (tiles - 1) * 256 :], preferred_element_type=F32)
    for j in range(nt):
        for part in range(2):
            block = kv[8 * j : 8 * j + 8, part * HD : (part + 1) * HD]
            p1[part * nt + j, pl.ds(rows, 16), :] = jnp.concatenate(
                [block, squares], axis=0
            ).astype(BF16)
    for n in range(tiles - 1):
        load_wq(n).wait()
        two = jnp.dot(xgv, wq_v[:, n * 256 : n * 256 + 256], preferred_element_type=F32)
        p1[2 * n, pl.ds(0, rows), :] = two[:, :HD].astype(BF16)
        p1[2 * n + 1, pl.ds(0, rows), :] = two[:, HD:].astype(BF16)
    start1()
    r1[ctx] = p1[ctx]

    _, start2, wait2, drain2 = exchange(1, lambda d: p2, lambda d: r2.at[d])
    wait1()
    total = r1[0].astype(F32)
    for d in range(1, nc):
        total = total + r1[d].astype(F32)
    square_row = jnp.sum(total[rows + 8 :], axis=0, keepdims=True)
    scale_row = lax.rsqrt(square_row / features + EPSILON)
    scale = row_to_column(scale_row, rows)
    scales[...] = jnp.broadcast_to(scale, (rows, LANES))
    kv_scale = scales[pl.ds(pl.multiple_of(8 * lax.rem(ctx, nt), 8), 8), :]
    done = jnp.concatenate(
        [total[:rows] * scale, total[rows : rows + 8] * kv_scale], axis=0
    ).astype(BF16)
    p2[...] = done
    r2[ctx] = done
    start2()

    send3, _, wait3, drain3 = exchange(2, lambda d: p3.at[d], lambda d: r3.at[d])
    for copy in later:
        copy.wait()
    wait2()
    for j in range(nt // 2):
        at = pl.ds(new_at + 16 * j, 16)
        for part, target in ((0, k_v), (1, vx)):
            pair = [r2[part * nt + 2 * j + i, pl.ds(rows, 8), :].astype(F32) for i in range(2)]
            target[at, pl.ds(0, HD)] = jnp.concatenate(pair, axis=0).astype(BF16)

    block_rows = HEADS_PER_BLOCK * rows
    blocks = heads // HEADS_PER_BLOCK
    chunk = min(512, smax)
    per_block = blocks * ctx // nc

    def scores(queries, start, length):
        return lax.dot_general(
            queries,
            k_v[pl.ds(start, length), :],
            (((1,), (1,)), ((), ())),
            preferred_element_type=F32,
        )

    def lane_max(best, values):
        for n in range(values.shape[1] // LANES):
            best = jnp.maximum(best, values[:, n * LANES : (n + 1) * LANES])
        return best

    def attend(b, carry):
        block = lax.rem(b + per_block, blocks)
        first = block * HEADS_PER_BLOCK
        queries = r2[pl.ds(first, HEADS_PER_BLOCK), pl.ds(0, rows), :].reshape(block_rows, HD)
        best = jnp.where(
            new_bias[...] == 0.0, scores(queries, new_at, LANES), NEGATIVE
        )
        s_v[:, new_at:] = best
        for i in range(slots):
            held = order_v[:, 0:1] == slots * ctx + i
            filled = lengths[slots * ctx + i]
            for n in range(smax // chunk):
                start = prefix + i * smax + n * chunk
                inside = iota((block_rows, chunk), 1) + n * chunk < filled
                values = jnp.where(held & inside, scores(queries, start, chunk), NEGATIVE)
                s_v[:, start : start + chunk] = values
                best = lane_max(best, values)
        for n in range(prefix // chunk):
            values = scores(queries, n * chunk, chunk)
            s_v[:, n * chunk : (n + 1) * chunk] = values
            best = lane_max(best, values)
        top = jnp.max(best, axis=1, keepdims=True)
        sums = jnp.zeros((block_rows, 2 * HD), F32)
        starts = [n * chunk for n in range(new_at // chunk)] + [new_at]
        for start in starts:
            length = chunk if start < new_at else LANES
            weights = jnp.exp2((s_v[:, start : start + length] - top) * SCALE2)
            sums = sums + jnp.dot(
                weights.astype(BF16),
                vx[pl.ds(start, length), :],
                preferred_element_type=F32,
            )
        weight_sum = sums[:, HD:]
        part = sums[:, :HD] / weight_sum
        level = top * SCALE2 + jnp.log2(weight_sum)
        for hh in range(HEADS_PER_BLOCK):
            at = slice(hh * rows, (hh + 1) * rows)
            head = first + hh
            p3[head] = jnp.concatenate(
                [part[at], in_three(column_to_row(level[at]))], axis=0
            ).astype(BF16)

            @pl.when(head != ctx)
            def _():
                send3(head).start()

        return carry

    lax.fori_loop(0, blocks, attend, 0)
    r3[ctx] = p3[ctx]

    def columns(d):
        return a4.at[:, pl.ds(pl.multiple_of(d * HD, HD), HD)]

    _, start4, wait4, drain4 = exchange(3, lambda d: p4, columns)
    wait3()
    levels = jnp.concatenate(
        [
            jnp.sum(r3[d, pl.ds(rows, 8), :].astype(F32), axis=0, keepdims=True)
            for d in range(nc)
        ],
        axis=0,
    )
    factors = jnp.exp2(levels - jnp.max(levels, axis=0, keepdims=True))
    factors = factors / jnp.sum(factors, axis=0, keepdims=True)
    padded = jnp.concatenate([factors, jnp.zeros((LANES - nc, LANES), F32)], axis=0)
    by_row = padded.T[:rows]
    joined = jnp.zeros((rows, HD), F32)
    for d in range(nc):
        joined = joined + by_row[:, d : d + 1] * r3[d, pl.ds(0, rows), :].astype(F32)
    attention = joined.astype(BF16)
    p4[...] = attention
    a4[:, pl.ds(pl.multiple_of(ctx * HD, HD), HD)] = attention
    start4()

    out_load.wait()
    wait4()
    whole = a4[...]
    for n in range(width // 256):
        terms = jnp.dot(whole, wo_v[:, n * 256 : n * 256 + 256], preferred_element_type=F32)
        p5[:, :, n * 256 : n * 256 + 256] = terms.reshape(nt, 8, 256).astype(BF16)

    def term_copy(d):
        return pltpu.make_async_remote_copy(
            src_ref=p5.at[d],
            dst_ref=r5.at[tp],
            send_sem=send_t.at[d],
            recv_sem=recv_t.at[tp],
            device_id={"tp": d},
        )

    def term_arrival(d):
        return pltpu.make_async_remote_copy(
            src_ref=r5.at[d],
            dst_ref=r5.at[d],
            send_sem=send_t.at[d],
            recv_sem=recv_t.at[d],
            device_id={"tp": d},
        )

    def start_terms(k, carry):
        term_copy(lax.rem(tp + k, nt)).start()
        return carry

    def wait_terms(k, carry):
        term_arrival(lax.rem(tp + k, nt)).wait_recv()
        return carry

    lax.fori_loop(1, nt, start_terms, 0)
    r5[tp] = p5[tp]

    @pl.when(sec == 1)
    def _():
        rest_copy.wait_recv()

    lax.fori_loop(1, nt, wait_terms, 0)
    passed = r5[0].astype(F32)
    for d in range(1, nt):
        passed = passed + r5[d].astype(F32)
    passed = passed + x_res[...]

    @pl.when(sec == 0)
    def _():
        gain_copy.wait_recv()
        xg6[...] = (passed * gain_next[...].astype(F32)).astype(BF16)
        total6 = jnp.sum(passed * passed, axis=1, keepdims=True)
        ss6[...] = jnp.broadcast_to(total6, (8, LANES))
        xn6[...] = passed

        def start(k, carry):
            for copy in row_copies(lax.rem(tp + k, nt)):
                copy.start()
            return carry

        lax.fori_loop(0, nt, start, 0)
        rest_copy.start()

    for t in range(STEPS):
        out[0, t] = passed[4 * t : 4 * t + 4]

    drain1()
    drain2()
    drain3()
    drain4()

    def drain_terms(k, carry):
        term_copy(lax.rem(tp + k, nt)).wait_send()
        return carry

    lax.fori_loop(1, nt, drain_terms, 0)

    @pl.when(sec == 0)
    def _():
        def wait(k, carry):
            for copy in row_copies(lax.rem(tp + k, nt)):
                copy.wait_send()
            return carry

        lax.fori_loop(0, nt, wait, 0)
        rest_copy.wait_send()


def on_device(nc, nt, tokens, gain, w_qkv, w_out, pre_k, pre_v, suf_k, suf_v, lengths, order):
    rows = 8 * nt
    model, wide = w_qkv.shape[1:]
    deep, width = w_out.shape[1:]
    prefix = pre_k.shape[2]
    slots, smax = suf_k.shape[2:4]
    keys = prefix + slots * smax + LANES
    block_rows = HEADS_PER_BLOCK * rows
    vmem, dma = pltpu.VMEM, pltpu.SemaphoreType.DMA
    anywhere = pl.BlockSpec(memory_space=pl.ANY)
    scalars = pl.BlockSpec(memory_space=pltpu.SMEM)
    return pl.pallas_call(
        functools.partial(kernel, nc, nt),
        out_shape=jax.ShapeDtypeStruct((1, STEPS, rows // STEPS // nt, width), F32),
        in_specs=[anywhere] * 8 + [scalars] * 2,
        out_specs=pl.BlockSpec(memory_space=pltpu.VMEM),
        scratch_shapes=[
            vmem(tokens.shape, BF16),
            vmem((1, model), BF16),
            vmem((1, model), BF16),
            vmem((model, wide), BF16),
            vmem((deep, width), BF16),
            vmem((keys, HD), BF16),
            vmem((keys, 2 * HD), BF16),
            vmem((nt, 8, model), BF16),
            vmem((8, width), F32),
            vmem((nt, 8, LANES), F32),
            vmem((nc, rows + 16, HD), BF16),
            vmem((nc, rows + 16, HD), BF16),
            vmem((rows, LANES), F32),
            vmem((rows + 8, HD), BF16),
            vmem((nc, rows + 8, HD), BF16),
            vmem((block_rows, LANES), jnp.int32),
            vmem((block_rows, LANES), F32),
            vmem((block_rows, keys), F32),
            vmem((nc, rows + 8, HD), BF16),
            vmem((nc, rows + 8, HD), BF16),
            vmem((rows, HD), BF16),
            vmem((rows, nc * HD), BF16),
            vmem((nt, 8, width), BF16),
            vmem((nt, 8, width), BF16),
            vmem((8, width), BF16),
            vmem((8, LANES), F32),
            vmem((8, width), F32),
            dma((5 + 2 * slots,)),
            dma((wide // 256,)),
            dma((4, nc)),
            dma((4, nc)),
            dma((nt,)),
            dma((nt,)),
            dma((3, nt)),
            dma((3, nt)),
            dma,
            dma,
        ],
        compiler_params=pltpu.CompilerParams(
            collective_id=0, has_side_effects=True, vmem_limit_bytes=60 * 1024 * 1024
        ),
    )(tokens, gain, w_qkv, w_out, pre_k, pre_v, suf_k, suf_v, lengths, order)


def solution(mesh):
    nc, nt = mesh.shape["ctx"], mesh.shape["tp"]
    in_specs = (
        P(None, None, "ctx"),
        P("section", "ctx"),
        P("section", "ctx", "tp"),
        P("section", "tp", "ctx"),
        P("section", "tp", "ctx", None),
        P("section", "tp", "ctx", None),
        P("section", "tp", "ctx", None, None),
        P("section", "tp", "ctx", None, None),
        P(),
        P(),
    )
    return jax.shard_map(
        functools.partial(on_device, nc, nt),
        mesh=mesh,
        in_specs=in_specs,
        out_specs=P("section", None, "tp", "ctx"),
        check_vma=False,
    )
```

```python
import functools
import math

import jax
import jax.numpy as jnp
from jax import lax
from jax.experimental import pallas as pl
from jax.experimental.pallas import tpu as pltpu
from jax.sharding import PartitionSpec as P

HD = 128
LANES = 128
STEPS = 2
EPSILON = 1e-05
NEGATIVE = -1e30
SCALE2 = HD ** (-0.5) * math.log2(math.e)
HEADS_PER_BLOCK = 8
CHUNKS = 2
CHUNK = 512
STRETCH = 2048
F32 = jnp.float32
BF16 = jnp.bfloat16


def iota(shape, dim):
    return lax.broadcasted_iota(jnp.int32, shape, dim)


def column_to_row(column):
    rows = column.shape[0]
    picked = jnp.where(iota((rows, LANES), 0) == iota((rows, LANES), 1), column, 0.0)
    return jnp.sum(picked, axis=0, keepdims=True)


def row_to_column(row, rows):
    spread = jnp.broadcast_to(row, (rows, LANES))
    picked = jnp.where(iota((rows, LANES), 0) == iota((rows, LANES), 1), spread, 0.0)
    return jnp.sum(picked, axis=1, keepdims=True)


def in_three(row):
    high = row.astype(BF16).astype(F32)
    rest = row - high
    middle = rest.astype(BF16).astype(F32)
    low = rest - middle
    which = iota((8, LANES), 0)
    block = jnp.where(which == 0, jnp.broadcast_to(high, (8, LANES)), 0.0)
    block = jnp.where(which == 1, jnp.broadcast_to(middle, (8, LANES)), block)
    return jnp.where(which == 2, jnp.broadcast_to(low, (8, LANES)), block)


def kernel(
    nc,
    nt,
    tokens,
    gain,
    w_qkv,
    w_out,
    pre_keys,
    pre_values,
    suf_keys,
    suf_values,
    lengths,
    order,
    out,
    tok_v,
    gain_v,
    gain_next,
    wq_v,
    wo_v,
    k_v,
    vx,
    xg,
    x_res,
    ssb,
    p1,
    r1,
    p2,
    r2,
    order_v,
    new_bias,
    s_v,
    best_v,
    p3,
    r3,
    p4,
    a4,
    p5,
    r5,
    xg6,
    ss6,
    xn6,
    load_sem,
    wq_sem,
    send_c,
    recv_c,
    send_t,
    recv_t,
    send_x,
    recv_x,
    send_g,
    recv_g,
):
    sec = lax.axis_index("section")
    tp = lax.axis_index("tp")
    ctx = lax.axis_index("ctx")
    rows = 8 * nt
    owners = nt // CHUNKS
    crows = rows // CHUNKS
    half = nc // 2
    heads = nc
    heads_at_once = min(HEADS_PER_BLOCK, heads)

    def slot(j):
        return j % CHUNKS * owners + j // CHUNKS

    tp_chunk = lax.rem(tp, CHUNKS)
    tp_slot = tp_chunk * owners + tp // CHUNKS
    model = wq_v.shape[0]
    prefix = pre_keys.shape[2]
    slots, smax = suf_keys.shape[2], suf_keys.shape[3]
    width = wo_v.shape[1]
    features = model * nc
    new_at = prefix + slots * smax
    tiles = wq_sem.shape[0]

    def load(source, target, k):
        return pltpu.make_async_copy(source, target, load_sem.at[k])

    def load_wq(n):
        cols = pl.ds(n * 256, 256)
        return pltpu.make_async_copy(
            w_qkv.at[0, :, cols], wq_v.at[:, cols], wq_sem.at[n]
        )

    barrier = pltpu.get_barrier_semaphore()

    def greet_ctx(k, carry):
        pl.semaphore_signal(barrier, inc=1, device_id={"ctx": lax.rem(ctx + k, nc)})
        return carry

    def greet_tp(k, carry):
        pl.semaphore_signal(barrier, inc=1, device_id={"tp": lax.rem(tp + k, nt)})
        return carry

    def greet_section(k, carry):
        pl.semaphore_signal(barrier, inc=1, device_id={"section": 1 - sec, "tp": k})
        return carry

    lax.fori_loop(1, nc, greet_ctx, 0)
    lax.fori_loop(1, nt, greet_tp, 0)
    lax.fori_loop(0, nt, greet_section, 0)

    loads = [
        load(tokens, tok_v, 0),
        load(gain, gain_v, 1),
    ]
    for copy in loads:
        copy.start()
    for n in [tiles - 1] + list(range(tiles - 1)):
        load_wq(n).start()
    later = [
        load(pre_keys.at[0, 0], k_v.at[pl.ds(0, prefix)], 2),
        load(pre_values.at[0, 0], vx.at[pl.ds(0, prefix), pl.ds(0, HD)], 3),
    ]
    for i in range(slots):
        at = pl.ds(prefix + i * smax, smax)
        later.append(load(suf_keys.at[0, 0, i], k_v.at[at], 4 + 2 * i))
        later.append(load(suf_values.at[0, 0, i], vx.at[at, pl.ds(0, HD)], 5 + 2 * i))
    out_load = load(w_out.at[0], wo_v, 4 + 2 * slots)
    for copy in later:
        copy.start()
    out_load.start()

    vx[:, HD:] = jnp.ones((vx.shape[0], HD), BF16)
    spare = LANES - crows
    for q in range(CHUNKS):
        at = pl.ds(new_at + q * LANES + crows, spare)
        k_v[at, :] = jnp.zeros((spare, HD), BF16)
        vx[at, pl.ds(0, HD)] = jnp.zeros((spare, HD), BF16)
    row_of = iota((crows, LANES), 0)
    lane_of = iota((crows, LANES), 1)
    batch_row = ((row_of >> 3) << 2) + (row_of & 3)
    second = (row_of & 4) == 4
    mine = (row_of & (nc - 1)) == ctx
    allowed = mine & ((lane_of == row_of) | (second & (lane_of == row_of - 4)))
    bias = jnp.where(allowed, 0.0, NEGATIVE)
    for q in range(CHUNKS):
        sample = jnp.zeros((crows, LANES), jnp.int32)
        for r in range(4 * owners):
            sample = jnp.where(batch_row == r, order[4 * (CHUNKS * (r // 4) + q) + r % 4], sample)
        for hh in range(heads):
            order_v[q, pl.ds(hh * crows, crows), :] = sample
    for hh in range(heads):
        new_bias[pl.ds(hh * crows, crows), :] = bias

    for copy in loads:
        copy.wait()

    @pl.when(sec == 0)
    def _():
        g = gain_v[...].astype(F32)
        for j in range(nt):
            x8 = jnp.concatenate(
                [tok_v[t, pl.ds(4 * j, 4), :].astype(F32) for t in range(STEPS)], axis=0
            )
            xg[slot(j)] = (x8 * g).astype(BF16)
            total = jnp.sum(x8 * x8, axis=1, keepdims=True)
            ssb[slot(j)] = jnp.broadcast_to(total, (8, LANES))

            @pl.when(tp == j)
            def _():
                x_res[...] = x8

    gain_copy = pltpu.make_async_remote_copy(
        src_ref=gain_v,
        dst_ref=gain_next,
        send_sem=send_g,
        recv_sem=recv_g,
        device_id={"section": 1 - sec},
    )

    def row_copies(k):
        return [
            pltpu.make_async_remote_copy(
                src_ref=xg6,
                dst_ref=xg.at[tp_slot],
                send_sem=send_x.at[0, k],
                recv_sem=recv_x.at[0, tp_slot],
                device_id={"section": 1 - sec, "tp": k},
            ),
            pltpu.make_async_remote_copy(
                src_ref=ss6,
                dst_ref=ssb.at[tp_slot],
                send_sem=send_x.at[1, k],
                recv_sem=recv_x.at[1, tp_slot],
                device_id={"section": 1 - sec, "tp": k},
            ),
        ]

    def row_arrivals(j):
        return [
            pltpu.make_async_remote_copy(
                src_ref=xg.at[j],
                dst_ref=xg.at[j],
                send_sem=send_x.at[0, j],
                recv_sem=recv_x.at[0, j],
                device_id={"section": 1 - sec, "tp": j},
            ),
            pltpu.make_async_remote_copy(
                src_ref=ssb.at[j],
                dst_ref=ssb.at[j],
                send_sem=send_x.at[1, j],
                recv_sem=recv_x.at[1, j],
                device_id={"section": 1 - sec, "tp": j},
            ),
        ]

    rest_copy = pltpu.make_async_remote_copy(
        src_ref=xn6,
        dst_ref=x_res,
        send_sem=send_x.at[2, 0],
        recv_sem=recv_x.at[2, 0],
        device_id={"section": 1 - sec},
    )


    high, low = ctx // half, lax.rem(ctx, half)
    peers = []
    for far in range(half // 2, -1, -1):
        for other in (1, 0):
            for step in sorted({far, half - far if far else 0}):
                if (other, step) != (0, 0):
                    at = lax.rem(high + other, 2) * half + lax.rem(low + step, half)
                    peers.append((other * half + step, at))

    def exchange(phase, source, target):
        def send(d):
            return pltpu.make_async_remote_copy(
                src_ref=source(d),
                dst_ref=target(ctx),
                send_sem=send_c.at[phase, d],
                recv_sem=recv_c.at[phase, ctx],
                device_id={"ctx": d},
            )

        def arrival(d):
            return pltpu.make_async_remote_copy(
                src_ref=target(d),
                dst_ref=target(d),
                send_sem=send_c.at[phase, d],
                recv_sem=recv_c.at[phase, d],
                device_id={"ctx": d},
            )

        def start_all():
            for _, d in peers:
                send(d).start()

        def wait_all():
            for _, d in reversed(peers):
                arrival(d).wait_recv()

        def drain():
            for _, d in peers:
                send(d).wait_send()

        return send, start_all, wait_all, drain

    drains = []

    def enter():
        @pl.when(sec == 0)
        def _():
            pl.semaphore_wait(barrier, nc - 1 + nt - 1 + nt)

    @pl.when(sec == 1)
    def _():
        pl.semaphore_wait(barrier, nc - 1 + nt - 1 + nt)
        gain_copy.start()
        gain_copy.wait_send()


    def project(q):
        mine1, theirs1 = p1.at[q], r1.at[q]
        _, start, wait, drain = exchange(
            4 * q, lambda d: mine1.at[d], lambda d: theirs1.at[d]
        )
        drains.append(drain)

        @pl.when(sec == 1)
        def _():
            for j in range(q * owners, (q + 1) * owners):
                for copy in row_arrivals(j):
                    copy.wait_recv()

        here = pl.ds(q * owners, owners)
        xgv = xg[here].reshape(crows, model)
        squares = in_three(column_to_row(ssb[here].reshape(crows, LANES)))
        if q == 0:
            load_wq(tiles - 1).wait()
        kv = jnp.dot(xgv, wq_v[:, (tiles - 1) * 256 :], preferred_element_type=F32)
        for i in range(half):
            for part in range(2):
                block = kv[4 * i : 4 * i + 4, part * HD : (part + 1) * HD]
                mine1[part * half + i, pl.ds(crows, 8), :] = jnp.concatenate(
                    [block, squares[:4]], axis=0
                ).astype(BF16)
        for n in range(tiles - 1):
            if q == 0:
                load_wq(n).wait()
            two = jnp.dot(
                xgv, wq_v[:, n * 256 : n * 256 + 256], preferred_element_type=F32
            )
            mine1[2 * n, pl.ds(0, crows), :] = two[:, :HD].astype(BF16)
            mine1[2 * n + 1, pl.ds(0, crows), :] = two[:, HD:].astype(BF16)
        if q == 0:
            enter()
        start()
        theirs1[ctx] = mine1[ctx]
        return wait

    def spread(q, wait1):
        theirs1, mine2, theirs2 = r1.at[q], p2.at[q], r2.at[q]
        _, start, wait, drain = exchange(4 * q + 1, lambda d: mine2, lambda d: theirs2.at[d])
        drains.append(drain)
        wait1()
        total = theirs1[0].astype(F32)
        for d in range(1, nc):
            total = total + theirs1[d].astype(F32)
        square_row = jnp.sum(total[crows + 4 :], axis=0, keepdims=True)
        scale_row = lax.rsqrt(square_row / features + EPSILON)
        scale = row_to_column(scale_row, crows)
        picked = iota((8, LANES), 1) == iota((8, LANES), 0) + 4 * lax.rem(ctx, half)
        picked = picked & (iota((8, LANES), 0) < 4)
        kv_scale = jnp.sum(
            jnp.where(picked, jnp.broadcast_to(scale_row, (8, LANES)), 0.0),
            axis=1,
            keepdims=True,
        )
        done = jnp.concatenate(
            [total[:crows] * scale, total[crows:] * kv_scale], axis=0
        ).astype(BF16)
        mine2[...] = done
        theirs2[ctx] = done
        start()
        return wait

    block_rows = heads_at_once * crows
    blocks = heads // heads_at_once
    chunk = min(CHUNK, smax)
    stretch = min(STRETCH, prefix)
    all_rows = heads * crows
    first_block = blocks * ctx // nc

    def lane_max(best, values):
        for n in range(values.shape[1] // LANES):
            best = jnp.maximum(best, values[:, n * LANES : (n + 1) * LANES])
        return best

    def scores(queries, start, length):
        return lax.dot_general(
            queries,
            k_v[pl.ds(start, length), :],
            (((1,), (1,)), ((), ())),
            preferred_element_type=F32,
        )

    def attend(q, wait2):
        theirs2, mine3, theirs3 = r2.at[q], p3.at[q], r3.at[q]
        send, _, wait, drain = exchange(
            4 * q + 2, lambda d: mine3.at[d], lambda d: theirs3.at[d]
        )
        drains.append(drain)
        if q == 0:
            for copy in later:
                copy.wait()
        wait2()
        fresh_at = new_at + q * LANES
        for part, target in ((0, k_v), (1, vx)):
            fresh = [
                theirs2[part * half + i, pl.ds(crows, 8), :].astype(F32)[:4]
                for i in range(half)
            ]
            target[pl.ds(fresh_at, crows), pl.ds(0, HD)] = jnp.concatenate(
                fresh, axis=0
            ).astype(BF16)

        queries = theirs2[:, pl.ds(0, crows), :].reshape(all_rows, HD)
        best_v[...] = jnp.where(
            new_bias[...] == 0.0, scores(queries, fresh_at, LANES), NEGATIVE
        )
        s_v[:, new_at:] = best_v[...]

        def own_suffix(i, carry):
            best = best_v[...]
            held = order_v[q, :, 0:1] == slots * ctx + i
            filled = lengths[slots * ctx + i]
            base = pl.multiple_of(prefix + i * smax, smax)
            for n in range(smax // chunk):
                inside = iota((all_rows, chunk), 1) + n * chunk < filled
                at = pl.ds(base + n * chunk, chunk)
                values = scores(queries, base + n * chunk, chunk)
                values = jnp.where(held & inside, values, NEGATIVE)
                s_v[:, at] = values
                best = lane_max(best, values)
            best_v[...] = best
            return carry

        lax.fori_loop(0, slots, own_suffix, 0)

        def shared_prefix(i, carry):
            best = best_v[...]
            base = pl.multiple_of(i * stretch, stretch)
            for n in range(stretch // chunk):
                values = scores(queries, base + n * chunk, chunk)
                s_v[:, pl.ds(base + n * chunk, chunk)] = values
                best = lane_max(best, values)
            best_v[...] = best
            return carry

        lax.fori_loop(0, prefix // stretch, shared_prefix, 0)

        def one_block(b, carry):
            first = lax.rem(b + first_block, blocks) * heads_at_once
            here = pl.ds(pl.multiple_of(first * crows, block_rows), block_rows)
            top = jnp.max(best_v[here], axis=1, keepdims=True)
            sums = jnp.zeros((block_rows, 2 * HD), F32)
            for start in [n * chunk for n in range(new_at // chunk)] + [new_at]:
                length = chunk if start < new_at else LANES
                source = start if start < new_at else fresh_at
                weights = jnp.exp2((s_v[here, start : start + length] - top) * SCALE2)
                sums = sums + jnp.dot(
                    weights.astype(BF16),
                    vx[pl.ds(source, length), :],
                    preferred_element_type=F32,
                )
            weight_sum = sums[:, HD:]
            part = sums[:, :HD] / weight_sum
            level = top * SCALE2 + jnp.log2(weight_sum)
            for hh in range(heads_at_once):
                at = slice(hh * crows, (hh + 1) * crows)
                head = first + hh
                mine3[head] = jnp.concatenate(
                    [part[at], in_three(column_to_row(level[at]))], axis=0
                ).astype(BF16)

                @pl.when(head != ctx)
                def _():
                    send(head).start()

            return carry

        lax.fori_loop(0, blocks, one_block, 0)
        theirs3[ctx] = mine3[ctx]
        return wait

    def join(q, wait3):
        theirs3, mine4, theirs4 = r3.at[q], p4.at[q], a4.at[q]

        def columns(d):
            return theirs4.at[:, pl.ds(pl.multiple_of(d * HD, HD), HD)]

        _, start, wait, drain = exchange(4 * q + 3, lambda d: mine4, columns)
        drains.append(drain)
        wait3()
        levels = jnp.concatenate(
            [
                jnp.sum(theirs3[d, pl.ds(crows, 8), :].astype(F32), axis=0, keepdims=True)
                for d in range(nc)
            ],
            axis=0,
        )
        factors = jnp.exp2(levels - jnp.max(levels, axis=0, keepdims=True))
        factors = factors / jnp.sum(factors, axis=0, keepdims=True)
        padded = jnp.concatenate([factors, jnp.zeros((LANES - nc, LANES), F32)], axis=0)
        by_row = padded.T[:crows]
        joined = jnp.zeros((crows, HD), F32)
        for d in range(nc):
            joined = joined + by_row[:, d : d + 1] * theirs3[d, pl.ds(0, crows), :].astype(F32)
        attention = joined.astype(BF16)
        mine4[...] = attention
        theirs4[:, pl.ds(pl.multiple_of(ctx * HD, HD), HD)] = attention
        start()
        return wait

    def term_copy(d):
        return pltpu.make_async_remote_copy(
            src_ref=p5.at[slot(d)],
            dst_ref=r5.at[tp],
            send_sem=send_t.at[d],
            recv_sem=recv_t.at[tp],
            device_id={"tp": d},
        )

    def term_arrival(d):
        return pltpu.make_async_remote_copy(
            src_ref=r5.at[d],
            dst_ref=r5.at[d],
            send_sem=send_t.at[d],
            recv_sem=recv_t.at[d],
            device_id={"tp": d},
        )

    def start_terms(d):
        @pl.when(d != tp)
        def _():
            term_copy(d).start()

    def expand(q, wait4):
        if q == 0:
            out_load.wait()
        wait4()
        whole = a4[q]
        for n in range(width // 256):
            cols = slice(n * 256, n * 256 + 256)
            terms = jnp.dot(whole, wo_v[:, cols], preferred_element_type=F32)
            p5[pl.ds(q * owners, owners), :, cols] = terms.reshape(owners, 8, 256).astype(BF16)
        for d in range(q, nt, CHUNKS):
            start_terms(d)

        @pl.when(tp_chunk == q)
        def _():
            finish()

    def finish():
        r5[tp] = p5[tp_slot]

        @pl.when(sec == 1)
        def _():
            rest_copy.wait_recv()

        for k in range(1, nt):
            term_arrival(lax.rem(tp + k, nt)).wait_recv()
        passed = r5[0].astype(F32)
        for d in range(1, nt):
            passed = passed + r5[d].astype(F32)
        passed = passed + x_res[...]

        @pl.when(sec == 0)
        def _():
            gain_copy.wait_recv()
            xg6[...] = (passed * gain_next[...].astype(F32)).astype(BF16)
            total = jnp.sum(passed * passed, axis=1, keepdims=True)
            ss6[...] = jnp.broadcast_to(total, (8, LANES))
            xn6[...] = passed
            for k in range(nt):
                for copy in row_copies(lax.rem(tp + k, nt)):
                    copy.start()
            rest_copy.start()

        for t in range(STEPS):
            out[0, t] = passed[4 * t : 4 * t + 4]

    waits = [None] * CHUNKS
    for stage in (project, spread, attend, join, expand):
        for q in range(CHUNKS):
            waits[q] = stage(q) if stage is project else stage(q, waits[q])

    for drain in drains:
        drain()
    for d in range(nt):

        @pl.when(d != tp)
        def _():
            term_copy(d).wait_send()

    @pl.when(sec == 0)
    def _():
        for k in range(nt):
            for copy in row_copies(k):
                copy.wait_send()
        rest_copy.wait_send()


def on_device(nc, nt, tokens, gain, w_qkv, w_out, pre_k, pre_v, suf_k, suf_v, lengths, order):
    rows = 8 * nt
    model, wide = w_qkv.shape[1:]
    deep, width = w_out.shape[1:]
    prefix = pre_k.shape[2]
    slots, smax = suf_k.shape[2:4]
    crows = rows // CHUNKS
    new_at = prefix + slots * smax
    keys = new_at + CHUNKS * LANES
    all_rows = nc * crows
    vmem, dma = pltpu.VMEM, pltpu.SemaphoreType.DMA
    anywhere = pl.BlockSpec(memory_space=pl.ANY)
    scalars = pl.BlockSpec(memory_space=pltpu.SMEM)
    return pl.pallas_call(
        functools.partial(kernel, nc, nt),
        out_shape=jax.ShapeDtypeStruct((1, STEPS, rows // STEPS // nt, width), F32),
        in_specs=[anywhere] * 8 + [scalars] * 2,
        out_specs=pl.BlockSpec(memory_space=pltpu.VMEM),
        scratch_shapes=[
            vmem(tokens.shape, BF16),
            vmem((1, model), BF16),
            vmem((1, model), BF16),
            vmem((model, wide), BF16),
            vmem((deep, width), BF16),
            vmem((keys, HD), BF16),
            vmem((keys, 2 * HD), BF16),
            vmem((nt, 8, model), BF16),
            vmem((8, width), F32),
            vmem((nt, 8, LANES), F32),
            vmem((CHUNKS, nc, crows + 8, HD), BF16),
            vmem((CHUNKS, nc, crows + 8, HD), BF16),
            vmem((CHUNKS, crows + 8, HD), BF16),
            vmem((CHUNKS, nc, crows + 8, HD), BF16),
            vmem((CHUNKS, all_rows, LANES), jnp.int32),
            vmem((all_rows, LANES), F32),
            vmem((all_rows, new_at + LANES), F32),
            vmem((all_rows, LANES), F32),
            vmem((CHUNKS, nc, crows + 8, HD), BF16),
            vmem((CHUNKS, nc, crows + 8, HD), BF16),
            vmem((CHUNKS, crows, HD), BF16),
            vmem((CHUNKS, crows, nc * HD), BF16),
            vmem((nt, 8, width), BF16),
            vmem((nt, 8, width), BF16),
            vmem((8, width), BF16),
            vmem((8, LANES), F32),
            vmem((8, width), F32),
            dma((5 + 2 * slots,)),
            dma((wide // 256,)),
            dma((4 * CHUNKS, nc)),
            dma((4 * CHUNKS, nc)),
            dma((nt,)),
            dma((nt,)),
            dma((3, nt)),
            dma((3, nt)),
            dma,
            dma,
        ],
        compiler_params=pltpu.CompilerParams(
            collective_id=0, has_side_effects=True, vmem_limit_bytes=60 * 1024 * 1024
        ),
    )(tokens, gain, w_qkv, w_out, pre_k, pre_v, suf_k, suf_v, lengths, order)


def solution(mesh):
    nc, nt = mesh.shape["ctx"], mesh.shape["tp"]
    in_specs = (
        P(None, None, "ctx"),
        P("section", "ctx"),
        P("section", "ctx", "tp"),
        P("section", "tp", "ctx"),
        P("section", "tp", "ctx", None),
        P("section", "tp", "ctx", None),
        P("section", "tp", "ctx", None, None),
        P("section", "tp", "ctx", None, None),
        P(),
        P(),
    )
    return jax.shard_map(
        functools.partial(on_device, nc, nt),
        mesh=mesh,
        in_specs=in_specs,
        out_specs=P("section", None, "tp", "ctx"),
        check_vma=False,
    )
```

```python
import functools
import math

import jax
import jax.numpy as jnp
from jax import lax
from jax.experimental import pallas as pl
from jax.experimental.pallas import tpu as pltpu
from jax.sharding import PartitionSpec as P

HD = 128
LANES = 128
STEPS = 2
EPSILON = 1e-05
NEGATIVE = -1e30
SCALE2 = HD ** (-0.5) * math.log2(math.e)
CHUNKS = 2
CHUNK = 512
F32 = jnp.float32
BF16 = jnp.bfloat16


def iota(shape, dim):
    return lax.broadcasted_iota(jnp.int32, shape, dim)


def column_to_row(column):
    rows = column.shape[0]
    picked = jnp.where(iota((rows, LANES), 0) == iota((rows, LANES), 1), column, 0.0)
    return jnp.sum(picked, axis=0, keepdims=True)


def row_to_column(row, rows):
    spread = jnp.broadcast_to(row, (rows, LANES))
    picked = jnp.where(iota((rows, LANES), 0) == iota((rows, LANES), 1), spread, 0.0)
    return jnp.sum(picked, axis=1, keepdims=True)


def in_three(row):
    high = row.astype(BF16).astype(F32)
    rest = row - high
    middle = rest.astype(BF16).astype(F32)
    low = rest - middle
    which = iota((8, LANES), 0)
    block = jnp.where(which == 0, jnp.broadcast_to(high, (8, LANES)), 0.0)
    block = jnp.where(which == 1, jnp.broadcast_to(middle, (8, LANES)), block)
    return jnp.where(which == 2, jnp.broadcast_to(low, (8, LANES)), block)


def kernel(
    nc,
    nt,
    tokens,
    gain,
    w_qkv,
    w_out,
    pre_keys,
    pre_values,
    suf_keys,
    suf_values,
    lengths,
    order,
    out,
    tok_v,
    gain_v,
    wq_v,
    wo_v,
    k_v,
    vx,
    xg,
    x_res,
    ssb,
    p1,
    r1,
    p2,
    r2,
    order_v,
    new_bias,
    s_v,
    best_v,
    p3,
    r3,
    p4,
    a4,
    p5,
    r5,
    xg6,
    ss6,
    xn6,
    xn_back,
    load_sem,
    wq_sem,
    send_c,
    recv_c,
    send_t,
    recv_t,
    send_x,
    recv_x,
    send_g,
    recv_g,
):
    sec = lax.axis_index("section")
    tp = lax.axis_index("tp")
    ctx = lax.axis_index("ctx")
    rows = 8 * nt
    owners = nt // CHUNKS
    crows = rows // CHUNKS
    half = nc // 2
    heads = nc
    heads_at_once = half

    def slot(j):
        return j % CHUNKS * owners + j // CHUNKS

    tp_chunk = lax.rem(tp, CHUNKS)
    tp_slot = tp_chunk * owners + tp // CHUNKS
    model = wq_v.shape[0]
    prefix = pre_keys.shape[2]
    slots, smax = suf_keys.shape[2], suf_keys.shape[3]
    width = wo_v.shape[1]
    features = model * nc
    new_at = prefix + slots * smax
    tiles = wq_sem.shape[0]

    high, low = ctx // half, lax.rem(ctx, half)

    def from_afar(count):
        return sorted(range(count), key=lambda step: -min(step, count - step))

    peers = [
        (other, lax.rem(high + other, 2) * half + lax.rem(low + step, half))
        for step in from_afar(half)
        for other in (1, 0)
        if (other, step) != (0, 0)
    ]
    pairs = half // 2
    tile_order = [
        lax.rem(high + other, 2) * pairs + lax.rem(low // 2 + step, pairs)
        for step in from_afar(pairs)
        for other in (1, 0)
    ]

    def load(source, target, k):
        return pltpu.make_async_copy(source, target, load_sem.at[k])

    def load_wq(n):
        cols = pl.ds(pl.multiple_of(n * 256, 256), 256)
        return pltpu.make_async_copy(
            w_qkv.at[0, :, cols], wq_v.at[:, cols], wq_sem.at[n]
        )

    barrier = pltpu.get_barrier_semaphore()
    for _, d in peers:
        pl.semaphore_signal(barrier, inc=1, device_id={"ctx": d})
    for k in from_afar(nt)[:-1]:
        pl.semaphore_signal(barrier, inc=1, device_id={"tp": lax.rem(tp + k, nt)})
    for k in range(nt):
        pl.semaphore_signal(barrier, inc=1, device_id={"section": 1 - sec, "tp": k})

    loads = [
        load(tokens, tok_v, 0),
        load(gain, gain_v, 1),
    ]
    for copy in loads:
        copy.start()
    for n in [tiles - 1] + tile_order:
        load_wq(n).start()
    later = [
        load(pre_keys.at[0, 0], k_v.at[pl.ds(0, prefix)], 2),
        load(pre_values.at[0, 0], vx.at[pl.ds(0, prefix), pl.ds(0, HD)], 3),
    ]
    for i in range(slots):
        at = pl.ds(prefix + i * smax, smax)
        later.append(load(suf_keys.at[0, 0, i], k_v.at[at], 4 + 2 * i))
        later.append(load(suf_values.at[0, 0, i], vx.at[at, pl.ds(0, HD)], 5 + 2 * i))
    out_load = load(w_out.at[0], wo_v, 4 + 2 * slots)
    vx[:, HD:] = jnp.ones((vx.shape[0], HD), BF16)
    spare = LANES - 16
    for q in range(CHUNKS):
        at = pl.ds(new_at + q * LANES + 16, spare)
        k_v[at, :] = jnp.zeros((spare, HD), BF16)
        vx[at, pl.ds(0, HD)] = jnp.zeros((spare, HD), BF16)
    row_of = iota((crows, LANES), 0)
    lane_of = iota((crows, LANES), 1)
    batch_row = ((row_of >> 3) << 2) + (row_of & 3)
    second = (row_of & 4) == 4
    mine = batch_row == ctx
    allowed = mine & ((lane_of == 0) | (second & (lane_of == 1)))
    bias = jnp.where(allowed, 0.0, NEGATIVE)
    for q in range(CHUNKS):
        sample = jnp.zeros((crows, LANES), jnp.int32)
        for r in range(4 * owners):
            sample = jnp.where(batch_row == r, order[4 * (CHUNKS * (r // 4) + q) + r % 4], sample)
        for hh in range(heads_at_once):
            order_v[q, pl.ds(hh * crows, crows), :] = sample
    for hh in range(heads_at_once):
        new_bias[pl.ds(hh * crows, crows), :] = bias

    for copy in loads:
        copy.wait()

    def first_rows(j):
        return jnp.concatenate(
            [tok_v[t, pl.ds(4 * j, 4), :].astype(F32) for t in range(STEPS)], axis=0
        )

    @pl.when(sec == 0)
    def _():
        g = gain_v[...].astype(F32)
        for j in range(nt):
            x8 = first_rows(j)
            xg[slot(j)] = (x8 * g).astype(BF16)
            total = jnp.sum(x8 * x8, axis=1, keepdims=True)
            ssb[slot(j)] = jnp.broadcast_to(total, (8, LANES))

    def term_copy(q, step):
        place = lax.rem(tp // CHUNKS + step, owners)
        d = CHUNKS * place + q
        return d, pltpu.make_async_remote_copy(
            src_ref=p5.at[q * owners + place],
            dst_ref=r5.at[sec, tp],
            send_sem=send_t.at[d],
            recv_sem=recv_t.at[sec, tp],
            device_id={"section": 1, "tp": d},
        )

    def each_term(q, act):
        for step in from_afar(owners):
            d, copy = term_copy(q, step)

            @pl.when((sec == 0) | (d != tp))
            def _():
                act(copy)

    def term_arrival(layer, d):
        return pltpu.make_async_remote_copy(
            src_ref=r5.at[layer, d],
            dst_ref=r5.at[layer, d],
            send_sem=send_t.at[d],
            recv_sem=recv_t.at[layer, d],
            device_id={"section": 1, "tp": d},
        )

    def row_copies(k):
        return [
            pltpu.make_async_remote_copy(
                src_ref=source,
                dst_ref=target.at[tp_slot],
                send_sem=send_x.at[i, k],
                recv_sem=recv_x.at[i, tp_slot],
                device_id={"tp": k},
            )
            for i, (source, target) in enumerate(((xg6, xg), (ss6, ssb)))
        ]

    def row_arrivals(j):
        return [
            pltpu.make_async_remote_copy(
                src_ref=target.at[j],
                dst_ref=target.at[j],
                send_sem=send_x.at[i, j],
                recv_sem=recv_x.at[i, j],
                device_id={"tp": j},
            )
            for i, target in enumerate((xg, ssb))
        ]

    back_copy = pltpu.make_async_remote_copy(
        src_ref=xn6,
        dst_ref=xn_back,
        send_sem=send_g,
        recv_sem=recv_g,
        device_id={"section": 1 - sec},
    )

    def exchange(phase, source, target):
        def send(d):
            return pltpu.make_async_remote_copy(
                src_ref=source(d),
                dst_ref=target(ctx),
                send_sem=send_c.at[phase, d],
                recv_sem=recv_c.at[phase, ctx],
                device_id={"ctx": d},
            )

        def arrival(d):
            return pltpu.make_async_remote_copy(
                src_ref=target(d),
                dst_ref=target(d),
                send_sem=send_c.at[phase, d],
                recv_sem=recv_c.at[phase, d],
                device_id={"ctx": d},
            )

        def start_all():
            for _, d in peers:
                send(d).start()

        def wait_all(columns=(0, 1)):
            for other, d in reversed(peers):
                if other in columns:
                    arrival(d).wait_recv()

        def drain():
            for _, d in peers:
                send(d).wait_send()

        return send, start_all, wait_all, drain

    drains = []

    def enter():
        @pl.when(sec == 0)
        def _():
            pl.semaphore_wait(barrier, nc - 1 + nt - 1 + nt)

    @pl.when(sec == 1)
    def _():
        for j in range(nt):

            @pl.when(tp == j)
            def _():
                x_res[...] = first_rows(j)

        pl.semaphore_wait(barrier, nc - 1 + nt - 1 + nt)
        for k in range(nt):
            term_arrival(0, k).wait_recv()
        passed = r5[0, 0].astype(F32)
        for d in range(1, nt):
            passed = passed + r5[0, d].astype(F32)
        passed = passed + x_res[...]
        rows6 = (passed * gain_v[...].astype(F32)).astype(BF16)
        total = jnp.sum(passed * passed, axis=1, keepdims=True)
        squares6 = jnp.broadcast_to(total, (8, LANES))
        xg6[...] = rows6
        ss6[...] = squares6
        xn6[...] = passed
        for k in from_afar(nt)[:-1]:
            for copy in row_copies(lax.rem(tp + k, nt)):
                copy.start()
        back_copy.start()
        xg[tp_slot] = rows6
        ssb[tp_slot] = squares6


    def project(q):
        mine1, theirs1 = p1.at[q], r1.at[q]
        send, _, wait, drain = exchange(
            4 * q, lambda d: mine1.at[d], lambda d: theirs1.at[d]
        )
        drains.append(drain)

        @pl.when(sec == 1)
        def _():
            for j in range(q * owners, (q + 1) * owners):

                @pl.when(j != tp_slot)
                def _():
                    for copy in row_arrivals(j):
                        copy.wait_recv()

        here = pl.ds(q * owners, owners)
        xgv = xg[here].reshape(crows, model)
        squares = in_three(column_to_row(ssb[here].reshape(crows, LANES)))
        if q == 0:
            load_wq(tiles - 1).wait()
        kv = jnp.dot(xgv, wq_v[:, (tiles - 1) * 256 :], preferred_element_type=F32)
        for i in range(nc):
            first = i // 4 * 8 + i % 4
            block = [
                kv[first + 4 * t : first + 4 * t + 1, part * HD : (part + 1) * HD]
                for part in range(2)
                for t in range(STEPS)
            ]
            mine1[i, pl.ds(crows, 8), :] = jnp.concatenate(
                [*block, squares[:4]], axis=0
            ).astype(BF16)
        ready = []
        for n in tile_order:
            if q == 0:
                load_wq(n).wait()
            cols = pl.ds(pl.multiple_of(n * 256, 256), 256)
            two = jnp.dot(xgv, wq_v[:, cols], preferred_element_type=F32)
            mine1[2 * n, pl.ds(0, crows), :] = two[:, :HD].astype(BF16)
            mine1[2 * n + 1, pl.ds(0, crows), :] = two[:, HD:].astype(BF16)
            if len(ready) == 2:
                if q == 0:
                    enter()
            if len(ready) >= 2:
                send(ready[-2]).start()
                send(ready[-1]).start()
            ready += [2 * n, 2 * n + 1]
        if q == 0 and len(ready) <= 2:
            enter()
        for d in ready[-2:]:

            @pl.when(d != ctx)
            def _():
                send(d).start()

        theirs1[ctx] = mine1[ctx]
        if q == 0:
            for copy in later:
                copy.start()
            out_load.start()
        return wait

    def spread(q, wait1):
        theirs1, mine2, theirs2 = r1.at[q], p2.at[q], r2.at[q]
        _, start, wait, drain = exchange(4 * q + 1, lambda d: mine2, lambda d: theirs2.at[d])
        drains.append(drain)
        wait1()
        total = theirs1[0].astype(F32)
        for d in range(1, nc):
            total = total + theirs1[d].astype(F32)
        square_row = jnp.sum(total[crows + 4 :], axis=0, keepdims=True)
        scale_row = lax.rsqrt(square_row / features + EPSILON)
        scale = row_to_column(scale_row, crows)
        place = (ctx // 4) * 8 + lax.rem(ctx, 4) + 4 * (iota((8, LANES), 0) & 1)
        kv_scale = jnp.sum(
            jnp.where(
                iota((8, LANES), 1) == place, jnp.broadcast_to(scale_row, (8, LANES)), 0.0
            ),
            axis=1,
            keepdims=True,
        )
        done = (total[:crows] * scale).astype(BF16)
        mine2[...] = done
        theirs2[ctx] = done
        start()
        fresh = total[crows:] * kv_scale
        lines = iota((16, LANES), 0)
        for part, target in ((0, k_v), (1, vx)):
            both = jnp.where(
                lines == 0,
                jnp.broadcast_to(fresh[2 * part : 2 * part + 1], (16, LANES)),
                jnp.broadcast_to(fresh[2 * part + 1 : 2 * part + 2], (16, LANES)),
            )
            target[pl.ds(new_at + q * LANES, 16), pl.ds(0, HD)] = jnp.where(
                lines < 2, both, 0.0
            ).astype(BF16)
        return wait

    block_rows = heads_at_once * crows
    chunk = min(CHUNK, smax)
    all_rows = heads * crows

    def lane_max(best, values):
        for n in range(values.shape[1] // LANES):
            best = jnp.maximum(best, values[:, n * LANES : (n + 1) * LANES])
        return best

    def scores(queries, start, length):
        return lax.dot_general(
            queries,
            k_v[pl.ds(start, length), :],
            (((1,), (1,)), ((), ())),
            preferred_element_type=F32,
        )

    def attend(q, wait2):
        theirs2, mine3, theirs3 = r2.at[q], p3.at[q], r3.at[q]
        send, _, wait, drain = exchange(
            4 * q + 2, lambda d: mine3.at[d], lambda d: theirs3.at[d]
        )
        drains.append(drain)
        if q == 0:
            for copy in later:
                copy.wait()
        early = q < CHUNKS - 1
        if not early:
            wait2()

        def first_of(b):
            return lax.rem(b + high + (0 if early else 1), 2) * heads_at_once

        fresh_at = new_at + q * LANES

        def score_block(b, carry):
            if early:

                @pl.when(b == 0)
                def _():
                    wait2((0,))

                @pl.when(b == 1)
                def _():
                    wait2((1,))

            first = first_of(b)
            here = pl.ds(pl.multiple_of(first * crows, block_rows), block_rows)
            queries = theirs2[pl.ds(first, heads_at_once)]
            queries = queries.reshape(block_rows, HD)
            best = jnp.full((block_rows, LANES), NEGATIVE, F32)
            for n in range(prefix // chunk):
                values = scores(queries, n * chunk, chunk)
                s_v[here, n * chunk : (n + 1) * chunk] = values
                best = lane_max(best, values)
            for i in range(slots):
                held = order_v[q, :, 0:1] == slots * ctx + i
                filled = lengths[slots * ctx + i]
                for n in range(smax // chunk):
                    start = prefix + i * smax + n * chunk
                    inside = iota((block_rows, chunk), 1) + n * chunk < filled
                    values = scores(queries, start, chunk)
                    values = jnp.where(held & inside, values, NEGATIVE)
                    s_v[here, start : start + chunk] = values
                    best = lane_max(best, values)
            values = jnp.where(
                new_bias[...] == 0.0, scores(queries, fresh_at, LANES), NEGATIVE
            )
            s_v[here, new_at:] = values
            best_v[here] = jnp.maximum(best, values)

            @pl.when(sec >= 0)
            def _():
                weigh_block(first, here)

            return carry

        def weigh_block(first, here):
            top = jnp.max(best_v[here], axis=1, keepdims=True)
            sums = jnp.zeros((block_rows, 2 * HD), F32)
            for start in [n * chunk for n in range(new_at // chunk)] + [new_at]:
                length = chunk if start < new_at else LANES
                source = start if start < new_at else fresh_at
                weights = jnp.exp2((s_v[here, start : start + length] - top) * SCALE2)
                sums = sums + jnp.dot(
                    weights.astype(BF16),
                    vx[pl.ds(source, length), :],
                    preferred_element_type=F32,
                )
            weight_sum = sums[:, HD:]
            part = sums[:, :HD] / weight_sum
            level = top * SCALE2 + jnp.log2(weight_sum)
            for hh in range(heads_at_once):
                at = slice(hh * crows, (hh + 1) * crows)
                head = first + hh
                mine3[head] = jnp.concatenate(
                    [part[at], in_three(column_to_row(level[at]))], axis=0
                ).astype(BF16)
            for step in from_afar(half)[:-1]:
                send(first + lax.rem(low + step, half)).start()

            @pl.when(first + low != ctx)
            def _():
                send(first + low).start()

        lax.fori_loop(0, 2, score_block, 0)
        theirs3[ctx] = mine3[ctx]
        return wait

    def join(q, wait3):
        theirs3, mine4, theirs4 = r3.at[q], p4.at[q], a4.at[q]

        def columns(d):
            return theirs4.at[:, pl.ds(pl.multiple_of(d * HD, HD), HD)]

        _, start, wait, drain = exchange(4 * q + 3, lambda d: mine4, columns)
        drains.append(drain)
        wait3()
        levels = jnp.concatenate(
            [
                jnp.sum(theirs3[d, pl.ds(crows, 8), :].astype(F32), axis=0, keepdims=True)
                for d in range(nc)
            ],
            axis=0,
        )
        factors = jnp.exp2(levels - jnp.max(levels, axis=0, keepdims=True))
        factors = factors / jnp.sum(factors, axis=0, keepdims=True)
        padded = jnp.concatenate([factors, jnp.zeros((LANES - nc, LANES), F32)], axis=0)
        by_row = padded.T[:crows]
        joined = jnp.zeros((crows, HD), F32)
        for d in range(nc):
            joined = joined + by_row[:, d : d + 1] * theirs3[d, pl.ds(0, crows), :].astype(F32)
        attention = joined.astype(BF16)
        mine4[...] = attention
        theirs4[:, pl.ds(pl.multiple_of(ctx * HD, HD), HD)] = attention
        start()
        return wait

    def expand(q, wait4):
        if q == 0:
            out_load.wait()
        wait4()
        whole = a4[q]
        for n in range(width // 256):
            cols = slice(n * 256, n * 256 + 256)
            terms = jnp.dot(whole, wo_v[:, cols], preferred_element_type=F32)
            p5[pl.ds(q * owners, owners), :, cols] = terms.reshape(owners, 8, 256).astype(BF16)
        each_term(q, lambda copy: copy.start())

    def finish():
        @pl.when(sec == 0)
        def _():
            back_copy.wait_recv()
            for t in range(STEPS):
                out[0, t] = xn_back[4 * t : 4 * t + 4]

        @pl.when(sec == 1)
        def _():
            r5[1, tp] = p5[tp_slot]
            for k in from_afar(nt)[::-1][1:]:
                term_arrival(1, lax.rem(tp + k, nt)).wait_recv()
            passed = r5[1, 0].astype(F32)
            for d in range(1, nt):
                passed = passed + r5[1, d].astype(F32)
            passed = passed + xn6[...]
            for t in range(STEPS):
                out[0, t] = passed[4 * t : 4 * t + 4]

    waits = [None] * CHUNKS
    for stage in (project, spread, attend, join, expand):
        for q in range(CHUNKS):
            waits[q] = stage(q) if stage is project else stage(q, waits[q])

    for drain in drains:
        drain()
    finish()
    for q in range(CHUNKS):
        each_term(q, lambda copy: copy.wait_send())

    @pl.when(sec == 1)
    def _():
        for k in from_afar(nt)[:-1]:
            for copy in row_copies(lax.rem(tp + k, nt)):
                copy.wait_send()
        back_copy.wait_send()


def on_device(nc, nt, tokens, gain, w_qkv, w_out, pre_k, pre_v, suf_k, suf_v, lengths, order):
    rows = 8 * nt
    model, wide = w_qkv.shape[1:]
    deep, width = w_out.shape[1:]
    prefix = pre_k.shape[2]
    slots, smax = suf_k.shape[2:4]
    crows = rows // CHUNKS
    new_at = prefix + slots * smax
    keys = new_at + CHUNKS * LANES
    all_rows = nc * crows
    vmem, dma = pltpu.VMEM, pltpu.SemaphoreType.DMA
    anywhere = pl.BlockSpec(memory_space=pl.ANY)
    scalars = pl.BlockSpec(memory_space=pltpu.SMEM)
    return pl.pallas_call(
        functools.partial(kernel, nc, nt),
        out_shape=jax.ShapeDtypeStruct((1, STEPS, rows // STEPS // nt, width), F32),
        in_specs=[anywhere] * 8 + [scalars] * 2,
        out_specs=pl.BlockSpec(memory_space=pltpu.VMEM),
        scratch_shapes=[
            vmem(tokens.shape, BF16),
            vmem((1, model), BF16),
            vmem((model, wide), BF16),
            vmem((deep, width), BF16),
            vmem((keys, HD), BF16),
            vmem((keys, 2 * HD), BF16),
            vmem((nt, 8, model), BF16),
            vmem((8, width), F32),
            vmem((nt, 8, LANES), F32),
            vmem((CHUNKS, nc, crows + 8, HD), BF16),
            vmem((CHUNKS, nc, crows + 8, HD), BF16),
            vmem((CHUNKS, crows, HD), BF16),
            vmem((CHUNKS, nc, crows, HD), BF16),
            vmem((CHUNKS, all_rows // 2, LANES), jnp.int32),
            vmem((all_rows // 2, LANES), F32),
            vmem((all_rows, new_at + LANES), F32),
            vmem((all_rows, LANES), F32),
            vmem((CHUNKS, nc, crows + 8, HD), BF16),
            vmem((CHUNKS, nc, crows + 8, HD), BF16),
            vmem((CHUNKS, crows, HD), BF16),
            vmem((CHUNKS, crows, nc * HD), BF16),
            vmem((nt, 8, width), BF16),
            vmem((2, nt, 8, width), BF16),
            vmem((8, width), BF16),
            vmem((8, LANES), F32),
            vmem((8, width), F32),
            vmem((8, width), F32),
            dma((5 + 2 * slots,)),
            dma((wide // 256,)),
            dma((4 * CHUNKS, nc)),
            dma((4 * CHUNKS, nc)),
            dma((nt,)),
            dma((2, nt)),
            dma((2, nt)),
            dma((2, nt)),
            dma,
            dma,
        ],
        compiler_params=pltpu.CompilerParams(
            collective_id=0, has_side_effects=True, vmem_limit_bytes=60 * 1024 * 1024
        ),
    )(tokens, gain, w_qkv, w_out, pre_k, pre_v, suf_k, suf_v, lengths, order)


def solution(mesh):
    nc, nt = mesh.shape["ctx"], mesh.shape["tp"]
    in_specs = (
        P(None, None, "ctx"),
        P("section", "ctx"),
        P("section", "ctx", "tp"),
        P("section", "tp", "ctx"),
        P("section", "tp", "ctx", None),
        P("section", "tp", "ctx", None),
        P("section", "tp", "ctx", None, None),
        P("section", "tp", "ctx", None, None),
        P(),
        P(),
    )
    return jax.shard_map(
        functools.partial(on_device, nc, nt),
        mesh=mesh,
        in_specs=in_specs,
        out_specs=P("section", None, "tp", "ctx"),
        check_vma=False,
    )
```
